32 devices in a mesh: zero: 2 (over core), cols: 4 (over y, x), ens: 4 (over z).
Axes of the slice: x: 2, y: 2, z: 4, core: 2. Of those that a mesh axis runs over, the one named last changes fastest.
Arguments:
- weight_gate: float32 [8192, 8192], P(('ens', 'zero'), 'cols'), parts along dimension 0, may hold values from -0.1875 to 0.1875
- moment_gate: float32 [8192, 8192], P(('ens', 'zero'), 'cols'), parts along dimension 0, may hold values from -0.125 to 0.125
- square_gate: float32 [8192, 8192], P(('ens', 'zero'), 'cols'), parts along dimension 0, may hold values from -0.125 to 0.125
- weight_up: float32 [8192, 8192], P(('ens', 'zero'), 'cols'), parts along dimension 0, may hold values from -0.1875 to 0.1875
- moment_up: float32 [8192, 8192], P(('ens', 'zero'), 'cols'), parts along dimension 0, may hold values from -0.125 to 0.125
- square_up: float32 [8192, 8192], P(('ens', 'zero'), 'cols'), parts along dimension 0, may hold values from -0.125 to 0.125
- norm_gain: float32 [8192], P(('ens', 'zero')), parts along dimension 0, may hold values from 0.25 to 1.75
Outputs:
- ready_gate: bfloat16 [8192, 8192], P('ens', 'cols'), parts along dimension 0
- ready_up: bfloat16 [8192, 8192], P('ens', 'cols'), parts along dimension 0
- factor_gate: float32 [32768], P(('ens', 'cols')), parts along dimension 0
- factor_up: float32 [32768], P(('ens', 'cols')), parts along dimension 0
The draws below stay inside these ranges and needn't reach their ends.
There are 4 independent parts, one for each index of `ens`. The reference program is written for one: setup_inputs(seed, part) draws one part's arguments, and reference() takes and returns one part's arrays. A program takes and returns all parts, laid end to end along the dimension named above; each array names one. Nothing has to cross between parts.
All inputs are finite; a program needn't handle non-finite values. Where the reference program divides by a largest or mean magnitude, that divisor is 1e-20 or more.
Results may differ from the reference program's by a relative error of at most 0.001.
Values may be sent and summed in bfloat16 or wider, within the bound.
No kernel may reach another device: no remote copies, remote signals or barrier semaphores. Data moves between devices by JAX's collectives and lax.ppermute only.
A program may use at most 128 MiB of HBM per device.

```python
import jax
import jax.numpy as jnp

D_MODEL = 2048
D_INNER = 8192


def raised(array, rng, source, target, parts, factor):
    owner, partner = [(jnp.arange(array.shape[axis_at]) // (array.shape[axis_at] // parts)).reshape([-1 if axis == axis_at else 1 for axis in range(array.ndim)]) for axis_at in (source, target)]
    chosen = jax.random.permutation(rng, parts)[partner]
    strong = (owner == chosen) | (owner == (partner + parts // 2) % parts)
    return jnp.where(strong, factor * array, array)


def steps_of(stream_key, extent, shards, smallest, high):
    loudness = 1.0
    for axis_at, shards_of in shards:
        heights = jax.random.uniform(jax.random.fold_in(jax.random.fold_in(stream_key, 6), axis_at), (shards_of,), jnp.float32, smallest / len(shards), high / len(shards))
        loudness = loudness * jnp.repeat(jnp.exp(heights), extent[axis_at] // shards_of).reshape((-1,) + (1,) * (len(extent) - 1 - axis_at))
    return loudness


def noise(rng, extent, spread, reach, cuts=(), kind=jnp.bfloat16):
    loudness = steps_of(rng, extent, cuts, -0.22, 0.18) if cuts else 1.0
    values = jax.random.normal(rng, extent, jnp.float32) * spread * loudness
    return jnp.minimum(jnp.maximum(values, -reach), reach).astype(kind)


def heavy_noise(own_key, extent, width, most, cuts, heavy, held_as=jnp.bfloat16):
    array = width * jax.random.normal(own_key, extent, jnp.float32)
    if cuts:
        array = array * steps_of(own_key, extent, cuts, -0.22, 0.18)
    return jnp.clip(raised(array, jax.random.fold_in(own_key, 3), *heavy), -most, most).astype(held_as)


def setup_inputs(seed: int = 0, part: int = 0) -> dict:
    keys = jax.random.split(jax.random.key(seed), 8)
    own_keys = jax.random.split(jax.random.fold_in(keys[7], part), 8)
    weight_gate = heavy_noise(own_keys[0], (D_MODEL, D_INNER), D_MODEL ** -0.5, 0.1875, ((0, 2), (1, 4)), (0, 1, 4, 2.0), jnp.float32)
    moment_gate = noise(own_keys[1], (D_MODEL, D_INNER), D_MODEL ** -0.5, 0.125, ((0, 2), (1, 4)), jnp.float32)
    square_gate = noise(own_keys[2], (D_MODEL, D_INNER), D_MODEL ** -0.5, 0.125, ((0, 2), (1, 4)), jnp.float32)
    weight_up = heavy_noise(own_keys[3], (D_MODEL, D_INNER), D_MODEL ** -0.5, 0.1875, ((0, 2), (1, 4)), (0, 1, 4, 2.0), jnp.float32)
    moment_up = noise(own_keys[4], (D_MODEL, D_INNER), D_MODEL ** -0.5, 0.125, ((0, 2), (1, 4)), jnp.float32)
    square_up = noise(own_keys[5], (D_MODEL, D_INNER), D_MODEL ** -0.5, 0.125, ((0, 2), (1, 4)), jnp.float32)
    norm_gain = jnp.clip(1.0 + 0.15 * jax.random.normal(own_keys[6], (D_MODEL,), jnp.float32), 0.25, 1.75)
    return {"weight_gate": weight_gate, "moment_gate": moment_gate, "square_gate": square_gate, "weight_up": weight_up, "moment_up": moment_up, "square_up": square_up, "norm_gain": norm_gain}


learn_rate = 0.2
hold_rate = 0.9


def reference(weight_gate, moment_gate, square_gate, weight_up, moment_up, square_up, norm_gain):
    hold_gate = hold_rate * moment_gate + square_gate
    latest_gate = weight_gate - learn_rate * hold_gate
    hold_up = hold_rate * moment_up + square_up
    latest_up = weight_up - learn_rate * hold_up
    latest_gained_gate = latest_gate * norm_gain[:, None]
    latest_gained_up = latest_up * norm_gain[:, None]
    factor_gate = jnp.max(jnp.abs(latest_gained_gate), axis=0)
    ready_gate = (latest_gained_gate / factor_gate).astype(jnp.bfloat16)
    factor_up = jnp.max(jnp.abs(latest_gained_up), axis=0)
    ready_up = (latest_gained_up / factor_up).astype(jnp.bfloat16)
    return ready_gate, ready_up, factor_gate, factor_up
```

```python
import functools

import jax
import jax.numpy as jnp
from jax import lax
from jax.experimental import pallas as pl
from jax.experimental.pallas import tpu as pltpu
from jax.sharding import PartitionSpec as P


learn_rate = 0.2
hold_rate = 0.9
LANES = 128
BLOCKS = 8
GROUP = 512
AHEAD = 4
MIB = 2**20
VM = pl.BlockSpec(memory_space=pltpu.VMEM)
HB = pl.BlockSpec(memory_space=pltpu.HBM)

PARTS = {
    "x0": ((0, 0, 9),),
    "b0": ((0, 9, 7), (1, 0, 3)),
    "x1": ((1, 3, 5),),
    "b1": ((1, 8, 7),),
    "x2": ((1, 15, 1),),
}
STEPS = (
    (("x0", "b0"), (), ()),
    (("x1", "b1"), (), ()),
    (("x2",), ("b0",), ()),
    ((), ("b1",), ("x0",)),
    ((), (), ("x1", "b0")),
    ((), (), ("x2", "b1")),
)


def pieces(name, cols):
    unit = cols // 16
    return [(t, a * unit, w * unit) for t, a, w in PARTS[name]]


def width(name, cols):
    return sum(w for _, _, w in pieces(name, cols))


def groups(w):
    return [(q, min(GROUP, w - q)) for q in range(0, w, GROUP)]


def loop(count, body, init):
    return lax.fori_loop(0, count, body, init, unroll=min(4, count))


def update_block(j, block, x, top, top_row, raw, first, rows, gain):
    for q, size in groups(x.shape[1]):
        lanes = pl.ds(q, size)
        wide = pl.ds(first + q, size)

        def body(i, high):
            r = j * block + i * 8
            at = (pl.ds(r, 8), lanes)
            scale = jnp.concatenate([gain[pl.ds(r, 8), :]] * (size // LANES), axis=1)
            hold = hold_rate * raw[pl.ds(r, 8), wide] + raw[pl.ds(rows + r, 8), wide]
            value = (x[at] - learn_rate * hold) * scale
            x[at] = value
            return jnp.maximum(high, jnp.abs(value))

        high = loop(block // 8, body, jnp.zeros((8, size), jnp.float32))
        if j:
            high = jnp.maximum(high, top[pl.ds(top_row, 8), lanes])
        top[pl.ds(top_row, 8), lanes] = high


def scale_block(j, block, source, inverse, target, first):
    for q, size in groups(source.shape[1]):
        lanes = pl.ds(q, size)
        scale = jnp.broadcast_to(inverse[:, q : q + size], (16, size))

        def body(i, _):
            r = j * block + i * 16
            target[pl.ds(first + r, 16), lanes] = (source[pl.ds(r, 16), lanes] * scale).astype(target.dtype)
            return 0

        loop(block // 16, body, 0)


def step(n, rows, cols, plan, flags, *refs):
    new, scaled, finished = plan
    opening, with_outs, fresh, last = flags
    refs = list(refs)

    def take(count):
        taken = refs[:count]
        del refs[:count]
        return taken

    block = rows // BLOCKS
    me = lax.axis_index("zero")
    used = sorted({t for name in new for t, _, _ in pieces(name, cols)})
    tensors = {t: take(3) for t in used}
    gain_in = take(1)[0] if new else None
    scale_in = {name: (take(1)[0], take(1)[0], take(n - 1)) for name in scaled}
    finish_in = {name: (take(1)[0] if name[0] == "x" else None, take(n - 1)) for name in finished}
    here_best = [name for name in scaled + finished if name in scaled or name[0] == "x"]
    past = [name for name in last if name not in here_best]
    old_best = dict(zip(past, take(len(past))))
    if with_outs and not fresh:
        take(2)
    gain = gain_in
    if opening:
        gain = take(1)[0]
    made = {name: take(1 if name[0] == "x" else 2) for name in new}
    owns = {name: take(1)[0] for name in scaled}
    best = {name: take(1)[0] for name in here_best}
    outs = take(2) if with_outs else None
    fac = take(2) if last else None
    if new:
        raw, load_sem = take(2)
    if opening:
        gain_row, gain_sem = take(2)
    stages = {name: take(1)[0] for name in finished if name[0] == "x"}
    if with_outs:
        out_sem = take(1)[0]

    if opening:
        fetch = pltpu.make_async_copy(gain_in, gain_row, gain_sem)
        fetch.start()

    def load(j):
        here = pl.ds(j * block, block)
        first = 0
        for name in new:
            own = 0
            for t, c0, w in pieces(name, cols):
                lanes = pl.ds(c0, w)
                side = pl.ds(first, w)
                for source, target in (
                    (tensors[t][0], made[name][0].at[here, pl.ds(own, w)]),
                    (tensors[t][1], raw.at[here, side]),
                    (tensors[t][2], raw.at[pl.ds(rows + j * block, block), side]),
                ):
                    pltpu.make_async_copy(source.at[here, lanes], target, load_sem.at[j]).start()
                first += w
                own += w

    for j in range(AHEAD if new else 0):
        load(j)

    sem_at = 0
    waits = []

    def put(source, row, count, name, sem):
        at = 0
        for t, c0, w in pieces(name, cols):
            pltpu.make_async_copy(
                source.at[:, pl.ds(at, w)], outs[t].at[pl.ds(row, count), pl.ds(c0, w)], out_sem.at[sem]
            ).start()
            at += w

    for name in finished:
        if name[0] == "b":
            for k, other in enumerate(finish_in[name][1]):
                put(other, lax.rem(me + 1 + k, n) * rows, rows, name, sem_at)
                waits.append((other, sem_at))
                sem_at += 1
    for name in scaled:
        x, top, tops = scale_in[name]
        high = top[...]
        for other in tops:
            high = jnp.maximum(high, other[...])
        high = jnp.max(high, axis=0, keepdims=True)
        best[name][...] = jnp.broadcast_to(high, best[name].shape)
        inverse = 1.0 / high
        for j in range(BLOCKS):
            scale_block(j, block, x, inverse, owns[name], 0)
            put(owns[name].at[pl.ds(j * block, block), :], me * rows + j * block, block, name, sem_at)
        waits.append((owns[name], sem_at))
        sem_at += 1
    for name in finished:
        if name[0] == "x":
            own, got = finish_in[name]
            sources = [own] + got
            high = own[pl.ds(rows, 8), :]
            for other in got:
                high = jnp.maximum(high, other[pl.ds(rows, 8), :])
            high = jnp.max(high, axis=0, keepdims=True)
            best[name][...] = jnp.broadcast_to(high, best[name].shape)
            inverse = 1.0 / high
            stage = stages[name]
            for s, source in enumerate(sources):
                for j in range(BLOCKS):
                    scale_block(j, block, source, inverse, stage, s * rows)
                    put(
                        stage.at[pl.ds(s * rows + j * block, block), :],
                        lax.rem(me + s, n) * rows + j * block,
                        block,
                        name,
                        sem_at,
                    )
            waits.append((stage, sem_at))
            sem_at += 1

    if opening:
        fetch.wait()
        for j in range(rows // LANES):
            gain[pl.ds(j * LANES, LANES), :] = jnp.broadcast_to(gain_row[j : j + 1, :], (LANES, LANES)).T
    for j in range(BLOCKS if new else 0):
        whole = raw.at[pl.ds(0, 3 * block), :]
        pltpu.make_async_copy(whole, whole, load_sem.at[j]).wait()
        if j + AHEAD < BLOCKS:
            load(j + AHEAD)
        first = 0
        for name in new:
            x = made[name][0]
            top, row = (x, rows) if name[0] == "x" else (made[name][1], 0)
            update_block(j, block, x, top, row, raw, first, rows, gain)
            first += width(name, cols)

    for name in last:
        high = best[name] if name in best else old_best[name]
        first = 0
        for t, c0, w in pieces(name, cols):
            for q in range(0, w, LANES):
                row = (c0 + q) // LANES
                fac[t][row : row + 1, :] = high[0:1, first + q : first + q + LANES]
            first += w
    for whole, sem in waits:
        pltpu.make_async_copy(whole, whole, out_sem.at[sem]).wait()


def per_device(n, weight_gate, moment_gate, square_gate, weight_up, moment_up, square_up, norm_gain):
    rows, cols = weight_gate.shape
    far = [
        pltpu.with_memory_space_constraint(v, pltpu.HBM)
        for v in (weight_gate, moment_gate, square_gate, weight_up, moment_up, square_up)
    ]
    gain = pltpu.with_memory_space_constraint(norm_gain.reshape(rows // LANES, LANES), pltpu.HBM)
    back = [[(i, (i - k) % n) for i in range(n)] for k in range(1, n)]
    outs = None
    own, top, tops, got, best = {}, {}, {}, {}, {}
    wide = {name: width(name, cols) for name in PARTS}

    def swap(value):
        return [lax.ppermute(value, "zero", pairs) for pairs in back]

    for s, (new, scaled, finished) in enumerate(STEPS):
        opening = s == 0
        with_outs = bool(scaled or finished)
        fresh = outs is None
        last = tuple(PARTS) if s == len(STEPS) - 1 else ()
        args, specs, shapes, scratch, aliases = [], [], [], [], {}

        def add(values, spec):
            args.extend(values)
            specs.extend([spec] * len(values))

        for t in sorted({t for name in new for t, _, _ in pieces(name, cols)}):
            add(far[3 * t : 3 * t + 3], HB)
        if new:
            add([gain], HB if opening else VM)
        for name in scaled:
            add([own[name], top[name]] + tops[name], VM)
        for name in finished:
            add(([own[name]] if name[0] == "x" else []) + got[name], VM)
        made_here = [name for name in scaled + finished if name in scaled or name[0] == "x"]
        old_best = [name for name in last if name not in made_here]
        add([best[name] for name in old_best], VM)
        if opening:
            shapes.append(pltpu.VMEM((rows, LANES), jnp.float32))
        for name in new:
            if name[0] == "x":
                shapes.append(pltpu.VMEM((rows + 8, wide[name]), jnp.float32))
            else:
                shapes.append(pltpu.VMEM((rows, wide[name]), jnp.float32))
                shapes.append(pltpu.VMEM((8, wide[name]), jnp.float32))
        shapes += [pltpu.VMEM((rows, wide[name]), jnp.bfloat16) for name in scaled]
        shapes += [pltpu.VMEM((8, wide[name]), jnp.float32) for name in made_here]
        out_specs = [VM] * len(shapes)
        total = sum(wide[name] for name in new)
        room = 2
        if new:
            scratch += [pltpu.VMEM((2 * rows, total), jnp.float32), pltpu.SemaphoreType.DMA((BLOCKS,))]
            room += 2 * rows * total * 4 // MIB
        if opening:
            scratch += [pltpu.VMEM((rows // LANES, LANES), jnp.float32), pltpu.SemaphoreType.DMA]
        for name in finished:
            if name[0] == "x":
                scratch.append(pltpu.VMEM((n * rows, wide[name]), jnp.bfloat16))
                room += n * rows * wide[name] * 2 // MIB + 1
        if with_outs:
            count = len(scaled) + sum(1 if name[0] == "x" else n - 1 for name in finished)
            scratch.append(pltpu.SemaphoreType.DMA((count,)))
            if not fresh:
                for q in range(2):
                    aliases[len(args) + q] = len(shapes) + q
                add(outs, HB)
            shapes += [jax.ShapeDtypeStruct((n * rows, cols), jnp.bfloat16)] * 2
            out_specs += [HB] * 2
        if last:
            shapes += [jax.ShapeDtypeStruct((cols // LANES, LANES), jnp.float32)] * 2
            out_specs += [VM] * 2
        result = list(
            pl.pallas_call(
                functools.partial(
                    step, n, rows, cols, (new, scaled, finished), (opening, with_outs, fresh, last)
                ),
                out_shape=shapes,
                in_specs=specs,
                out_specs=out_specs,
                scratch_shapes=scratch,
                input_output_aliases=aliases,
                cost_estimate=pl.CostEstimate(flops=10**8, bytes_accessed=16 * MIB, transcendentals=0),
                compiler_params=pltpu.CompilerParams(vmem_limit_bytes=room * MIB),
            )(*args)
        )
        if opening:
            gain = result.pop(0)
        for name in new:
            own[name] = result.pop(0)
            if name[0] == "b":
                top[name] = result.pop(0)
                tops[name] = swap(top[name])
            else:
                got[name] = swap(own[name])
        for name in scaled:
            got[name] = swap(result.pop(0))
        for name in made_here:
            best[name] = result.pop(0)
        if with_outs:
            outs = [result.pop(0), result.pop(0)]
    return (outs[0], outs[1], result[0].reshape(-1), result[1].reshape(-1))


def solution(mesh):
    def body(*values):
        return per_device(mesh.shape["zero"], *values)

    split = P(("ens", "zero"), "cols")
    return jax.shard_map(
        body,
        mesh=mesh,
        in_specs=(split,) * 6 + (P(("ens", "zero")),),
        out_specs=(P("ens", "cols"), P("ens", "cols"), P(("ens", "cols")), P(("ens", "cols"))),
        check_vma=False,
    )
```

```python
import functools

import jax
import jax.numpy as jnp
from jax import lax
from jax.experimental import pallas as pl
from jax.experimental.pallas import tpu as pltpu
from jax.sharding import PartitionSpec as P


learn_rate = 0.2
hold_rate = 0.9
LANES = 128
BLOCKS = 16
ROWS = 16
GROUP = 512
AHEAD = 16
MIB = 2**20
VM = pl.BlockSpec(memory_space=pltpu.VMEM)
HB = pl.BlockSpec(memory_space=pltpu.HBM)

PARTS = {
    "x0": ((0, 0, 13),),
    "x1": ((0, 13, 3),),
    "b1": ((1, 0, 16),),
}
SENDS = {"b1": (10, 6)}
STEPS = (
    (("x0",), (), (), ()),
    (("x1", "b1"), (), (), ()),
    ((), ("b1",), (), ()),
    ((), (), ("b1.0", "b1.1"), ("x0",)),
    ((), (), (), ("x1", "b1.0")),
    ((), (), (), ("b1.1",)),
)


def sends(name):
    return [f"{name}.{k}" for k in range(len(SENDS[name]))]


def pieces(name, cols):
    unit = cols // 16
    part, _, k = name.partition(".")
    spans = PARTS[part]
    if k:
        skip, left, spans = sum(SENDS[part][: int(k)]), SENDS[part][int(k)], []
        for t, a, w in PARTS[part]:
            gone = min(skip, w)
            kept = min(left, w - gone)
            skip, left = skip - gone, left - kept
            if kept:
                spans.append((t, a + gone, kept))
    return [(t, a * unit, w * unit) for t, a, w in spans]


def width(name, cols):
    return sum(w for _, _, w in pieces(name, cols))


def blocks_of(rows):
    return min(BLOCKS, rows // ROWS)


def groups(w):
    return [(q, min(GROUP, w - q)) for q in range(0, w, GROUP)]


def loop(count, body, init):
    return lax.fori_loop(0, count, body, init, unroll=min(4, count))


def update_block(j, block, x, top, top_row, raw, first, rows, gain):
    for q, size in groups(x.shape[1]):
        lanes = pl.ds(q, size)
        wide = pl.ds(first + q, size)

        def body(i, high):
            r = pl.multiple_of(j * block + i * 8, 8)
            at = (pl.ds(r, 8), lanes)
            scale = jnp.concatenate([gain[pl.ds(r, 8), :]] * (size // LANES), axis=1)
            hold = hold_rate * raw[pl.ds(r, 8), wide] + raw[pl.ds(rows + r, 8), wide]
            value = (x[at] - learn_rate * hold) * scale
            x[at] = value
            return jnp.maximum(high, jnp.abs(value))

        top[pl.ds(top_row, 8), lanes] = loop(block // 8, body, top[pl.ds(top_row, 8), lanes])


def scale_block(j, block, source, side, inverse, target, first):
    for q, size in groups(target.shape[1]):
        lanes = pl.ds(q, size)
        wide = pl.ds(side + q, size)
        scale = jnp.broadcast_to(inverse[:, side + q : side + q + size], (16, size))

        def body(i, _):
            r = pl.multiple_of(j * block + i * 16, 16)
            target[pl.ds(first + r, 16), lanes] = (source[pl.ds(r, 16), wide] * scale).astype(target.dtype)
            return 0

        loop(block // 16, body, 0)


def step(n, rows, cols, plan, flags, *refs):
    new, scaled, owned, finished = plan
    opening, with_outs, fresh, last = flags
    refs = list(refs)

    def take(count):
        taken = refs[:count]
        del refs[:count]
        return taken

    count = blocks_of(rows)
    block = rows // count
    ahead = min(AHEAD, count)
    me = lax.axis_index("zero")
    used = sorted({t for name in new for t, _, _ in pieces(name, cols)})
    tensors = {t: take(3) for t in used}
    gain_in = take(1)[0] if new else None
    scale_in = {name: (take(1)[0], take(1)[0], take(n - 1)) for name in scaled}
    own_in = {name: take(1)[0] for name in owned}
    finish_in = {name: (take(1)[0] if name[0] == "x" else None, take(n - 1)) for name in finished}
    here_best = [name for name in scaled + finished if name in scaled or name[0] == "x"]
    past = [name for name in last if name not in here_best]
    old_best = dict(zip(past, take(len(past))))
    if with_outs and not fresh:
        take(2)
    gain = gain_in
    if opening:
        gain = take(1)[0]
    made = {name: take(1 if name[0] == "x" else 2) for name in new}
    owns = {name: take(len(SENDS[name])) for name in scaled}
    best = {name: take(1)[0] for name in here_best}
    outs = take(2) if with_outs else None
    fac_out = take(2) if last else None
    total = sum(width(name, cols) for name in new)
    if new:
        raw, load_sem = take(2)
    if opening:
        gain_row, gain_sem = take(2)
    stages = {name: take(1)[0] for name in finished if name[0] == "x"}
    if with_outs:
        out_sem = take(1)[0]
    if last:
        fac, fac_sem = take(2)

    if opening:
        fetch = pltpu.make_async_copy(gain_in, gain_row, gain_sem)
        fetch.start()
    spans = []
    first = 0
    for name in new:
        for t, c0, w in pieces(name, cols):
            if spans and spans[-1][0] == t and spans[-1][1] + spans[-1][2] == c0:
                spans[-1][2] += w
            else:
                spans.append([t, c0, w, first])
            first += w

    def load(j):
        here = pl.ds(j * block, block)
        for name in new:
            own = 0
            for t, c0, w in pieces(name, cols):
                target = made[name][0].at[here, pl.ds(own, w)]
                pltpu.make_async_copy(tensors[t][0].at[here, pl.ds(c0, w)], target, load_sem.at[j]).start()
                own += w
        for t, c0, w, side in spans:
            for k in range(2):
                target = raw.at[pl.ds(k * rows + j * block, block), pl.ds(side, w)]
                pltpu.make_async_copy(tensors[t][1 + k].at[here, pl.ds(c0, w)], target, load_sem.at[j]).start()

    if new:
        lax.fori_loop(0, ahead, lambda j, _: (load(j), 0)[1], 0)

    sem_at = 0
    waits = []

    def put(source, row, height, name, sem):
        at = 0
        for t, c0, w in pieces(name, cols):
            pltpu.make_async_copy(
                source.at[:, pl.ds(at, w)], outs[t].at[pl.ds(row, height), pl.ds(c0, w)], out_sem.at[sem]
            ).start()
            at += w

    for name in finished:
        if name[0] == "b":
            for k, other in enumerate(finish_in[name][1]):
                put(other, lax.rem(me + 1 + k, n) * rows, rows, name, sem_at)
                waits.append((other, sem_at))
                sem_at += 1
    for name in scaled:
        x, top, tops = scale_in[name]
        high = top[...]
        for other in tops:
            high = jnp.maximum(high, other[...])
        high = jnp.max(high, axis=0, keepdims=True)
        best[name][...] = jnp.broadcast_to(high, best[name].shape)
        inverse = 1.0 / high

        side = 0
        for target in owns[name]:

            def scale_own(j, _):
                scale_block(j, block, x, side, inverse, target, 0)
                return 0

            lax.fori_loop(0, count, scale_own, 0)
            side += target.shape[1]
    for name in owned:
        put(own_in[name], me * rows, rows, name, sem_at)
        waits.append((own_in[name], sem_at))
        sem_at += 1
    for name in finished:
        if name[0] == "x":
            own, got = finish_in[name]
            sources = [own] + got
            high = own[pl.ds(rows, 8), :]
            for other in got:
                high = jnp.maximum(high, other[pl.ds(rows, 8), :])
            high = jnp.max(high, axis=0, keepdims=True)
            best[name][...] = jnp.broadcast_to(high, best[name].shape)
            inverse = 1.0 / high
            stage = stages[name]
            for s, source in enumerate(sources):

                def scale_both(j, _):
                    scale_block(j, block, source, 0, inverse, stage, s * rows)
                    row = lax.rem(me + s, n) * rows + j * block
                    put(stage.at[pl.ds(s * rows + j * block, block), :], row, block, name, sem_at)
                    return 0

                lax.fori_loop(0, count, scale_both, 0)
            waits.append((stage, sem_at))
            sem_at += 1

    if opening:
        fetch.wait()

        def spread(j, _):
            gain[pl.ds(j * LANES, LANES), :] = jnp.broadcast_to(gain_row[pl.ds(j, 1), :], (LANES, LANES)).T
            return 0

        lax.fori_loop(0, rows // LANES, spread, 0)

    def one(j, _):
        whole = raw.at[pl.ds(0, 3 * block), :]
        pltpu.make_async_copy(whole, whole, load_sem.at[j]).wait()

        @pl.when(j + ahead < count)
        def _():
            load(j + ahead)

        first = 0
        for name in new:
            x = made[name][0]
            top, row = (x, rows) if name[0] == "x" else (made[name][1], 0)
            update_block(j, block, x, top, row, raw, first, rows, gain)
            first += width(name, cols)
        return 0

    if new:
        for name in new:
            top, row = (made[name][0], rows) if name[0] == "x" else (made[name][1], 0)
            top[pl.ds(row, 8), :] = jnp.zeros((8, top.shape[1]), jnp.float32)
        lax.fori_loop(0, count, one, 0)

    for name in last:
        high = best[name] if name in best else old_best[name]
        first = 0
        for t, c0, w in pieces(name, cols):
            for q in range(0, w, LANES):
                row = (c0 + q) // LANES
                fac[t, row : row + 1, :] = high[0:1, first + q : first + q + LANES]
            first += w
    if last:
        fac_copies = [pltpu.make_async_copy(fac.at[t], fac_out[t], fac_sem.at[t]) for t in range(2)]
        for copy in fac_copies:
            copy.start()
        for copy in fac_copies:
            copy.wait()
    for whole, sem in waits:
        pltpu.make_async_copy(whole, whole, out_sem.at[sem]).wait()


def per_device(n, weight_gate, moment_gate, square_gate, weight_up, moment_up, square_up, norm_gain):
    rows, cols = weight_gate.shape
    far = [
        pltpu.with_memory_space_constraint(v, pltpu.HBM)
        for v in (weight_gate, moment_gate, square_gate, weight_up, moment_up, square_up)
    ]
    gain = pltpu.with_memory_space_constraint(norm_gain.reshape(rows // LANES, LANES), pltpu.HBM)
    back = [[(i, (i - k) % n) for i in range(n)] for k in range(1, n)]
    outs = None
    own, top, tops, got, best = {}, {}, {}, {}, {}
    wide = {name: width(name, cols) for name in [*PARTS, *(v for k in SENDS for v in sends(k))]}

    def swap(value):
        return [lax.ppermute(value, "zero", pairs) for pairs in back]

    for s, (new, scaled, owned, finished) in enumerate(STEPS):
        opening = s == 0
        with_outs = bool(owned or finished)
        fresh = outs is None
        last = tuple(PARTS) if s == len(STEPS) - 1 else ()
        args, specs, shapes, scratch, aliases = [], [], [], [], {}

        def add(values, spec):
            args.extend(values)
            specs.extend([spec] * len(values))

        for t in sorted({t for name in new for t, _, _ in pieces(name, cols)}):
            add(far[3 * t : 3 * t + 3], HB)
        if new:
            add([gain], HB if opening else VM)
        for name in scaled:
            add([own[name], top[name]] + tops[name], VM)
        add([own[name] for name in owned], VM)
        for name in finished:
            add(([own[name]] if name[0] == "x" else []) + got[name], VM)
        made_here = [name for name in scaled + finished if name in scaled or name[0] == "x"]
        old_best = [name for name in last if name not in made_here]
        add([best[name] for name in old_best], VM)
        if opening:
            shapes.append(pltpu.VMEM((rows, LANES), jnp.float32))
        for name in new:
            if name[0] == "x":
                shapes.append(pltpu.VMEM((rows + 8, wide[name]), jnp.float32))
            else:
                shapes.append(pltpu.VMEM((rows, wide[name]), jnp.float32))
                shapes.append(pltpu.VMEM((8, wide[name]), jnp.float32))
        shapes += [pltpu.VMEM((rows, wide[send]), jnp.bfloat16) for name in scaled for send in sends(name)]
        shapes += [pltpu.VMEM((8, wide[name]), jnp.float32) for name in made_here]
        out_specs = [VM] * len(shapes)
        total = sum(wide[name] for name in new)
        room = 2
        if new:
            scratch += [pltpu.VMEM((2 * rows, total), jnp.float32), pltpu.SemaphoreType.DMA((blocks_of(rows),))]
            room += 2 * rows * total * 4 // MIB
        if opening:
            scratch += [pltpu.VMEM((rows // LANES, LANES), jnp.float32), pltpu.SemaphoreType.DMA]
        for name in finished:
            if name[0] == "x":
                scratch.append(pltpu.VMEM((n * rows, wide[name]), jnp.bfloat16))
                room += n * rows * wide[name] * 2 // MIB + 1
        if with_outs:
            count = len(owned) + sum(1 if name[0] == "x" else n - 1 for name in finished)
            scratch.append(pltpu.SemaphoreType.DMA((count,)))
            if not fresh:
                for q in range(2):
                    aliases[len(args) + q] = len(shapes) + q
                add(outs, HB)
            shapes += [jax.ShapeDtypeStruct((n * rows, cols), jnp.bfloat16)] * 2
            out_specs += [HB] * 2
        if last:
            shapes += [jax.ShapeDtypeStruct((cols // LANES, LANES), jnp.float32)] * 2
            out_specs += [HB] * 2
            scratch += [pltpu.VMEM((2, cols // LANES, LANES), jnp.float32), pltpu.SemaphoreType.DMA((2,))]
        result = list(
            pl.pallas_call(
                functools.partial(
                    step, n, rows, cols, (new, scaled, owned, finished), (opening, with_outs, fresh, last)
                ),
                out_shape=shapes,
                in_specs=specs,
                out_specs=out_specs,
                scratch_shapes=scratch,
                input_output_aliases=aliases,
                cost_estimate=pl.CostEstimate(flops=10**8, bytes_accessed=16 * MIB, transcendentals=0),
                compiler_params=pltpu.CompilerParams(vmem_limit_bytes=room * MIB),
            )(*args)
        )
        if opening:
            gain = result.pop(0)
        for name in new:
            own[name] = result.pop(0)
            if name[0] == "b":
                top[name] = result.pop(0)
                tops[name] = swap(top[name])
            else:
                got[name] = swap(own[name])
        for name in scaled:
            for send in sends(name):
                own[send] = result.pop(0)
                got[send] = swap(own[send])
        for name in made_here:
            best[name] = result.pop(0)
        if with_outs:
            outs = [result.pop(0), result.pop(0)]
    return (outs[0], outs[1], result[0].reshape(-1), result[1].reshape(-1))


def solution(mesh):
    def body(*values):
        return per_device(mesh.shape["zero"], *values)

    split = P(("ens", "zero"), "cols")
    return jax.shard_map(
        body,
        mesh=mesh,
        in_specs=(split,) * 6 + (P(("ens", "zero")),),
        out_specs=(P("ens", "cols"), P("ens", "cols"), P(("ens", "cols")), P(("ens", "cols"))),
        check_vma=False,
    )
```

```python
import functools

import jax
import jax.numpy as jnp
from jax import lax
from jax.experimental import pallas as pl
from jax.experimental.pallas import tpu as pltpu
from jax.sharding import PartitionSpec as P


learn_rate = 0.2
hold_rate = 0.9
LANES = 128
BLOCKS = 16
ROWS = 16
GROUP = 512
AHEAD = 16
NEAR = (5,)
MIB = 2**20
VM = pl.BlockSpec(memory_space=pltpu.VMEM)
HB = pl.BlockSpec(memory_space=pltpu.HBM)

PARTS = {
    "x0": ((0, 0, 13),),
    "x1": ((0, 13, 3),),
    "b1": ((1, 0, 16),),
}
SENDS = {"b1": (10, 6)}
STEPS = (
    (("x0",), (), (), ()),
    (("x1", "b1"), (), (), ()),
    ((), ("b1",), (), ()),
    ((), (), ("b1.0", "b1.1"), ("x0",)),
    ((), (), (), ("x1", "b1.0")),
    ((), (), (), ("b1.1",)),
)


def sends(name):
    return [f"{name}.{k}" for k in range(len(SENDS[name]))]


def pieces(name, cols):
    unit = cols // 16
    part, _, k = name.partition(".")
    spans = PARTS[part]
    if k:
        skip, left, spans = sum(SENDS[part][: int(k)]), SENDS[part][int(k)], []
        for t, a, w in PARTS[part]:
            gone = min(skip, w)
            kept = min(left, w - gone)
            skip, left = skip - gone, left - kept
            if kept:
                spans.append((t, a + gone, kept))
    return [(t, a * unit, w * unit) for t, a, w in spans]


def width(name, cols):
    return sum(w for _, _, w in pieces(name, cols))


def blocks_of(rows):
    return min(BLOCKS, rows // ROWS)


def groups(w):
    return [(q, min(GROUP, w - q)) for q in range(0, w, GROUP)]


def loop(count, body, init):
    return lax.fori_loop(0, count, body, init, unroll=min(8, count))


def update_block(j, block, x, top, top_row, raw, first, rows, gain, near):
    for q, size in groups(x.shape[1]):
        lanes = pl.ds(q, size)
        wide = pl.ds(first + q, size)

        def body(i, high):
            r = pl.multiple_of(j * block + i * 8, 8)
            at = (pl.ds(r, 8), lanes)
            scale = jnp.concatenate([gain[pl.ds(r, 8), :]] * (size // LANES), axis=1)
            if near is None:
                square = raw[pl.ds(rows + r, 8), wide]
            else:
                square = near[0][pl.ds(r, 8), pl.ds(near[1] + q, size)]
            hold = hold_rate * raw[pl.ds(r, 8), wide] + square
            value = (x[at] - learn_rate * hold) * scale
            x[at] = value
            return jnp.maximum(high, jnp.abs(value))

        top[pl.ds(top_row, 8), lanes] = loop(block // 8, body, top[pl.ds(top_row, 8), lanes])


def scale_block(j, block, source, side, inverse, target, first):
    for q, size in groups(target.shape[1]):
        lanes = pl.ds(q, size)
        wide = pl.ds(side + q, size)
        scale = jnp.broadcast_to(inverse[:, side + q : side + q + size], (16, size))

        def body(i, _):
            r = pl.multiple_of(j * block + i * 16, 16)
            target[pl.ds(first + r, 16), lanes] = (source[pl.ds(r, 16), wide] * scale).astype(target.dtype)
            return 0

        loop(block // 16, body, 0)


def step(n, rows, cols, plan, flags, *refs):
    new, scaled, owned, finished = plan
    opening, with_outs, fresh, last = flags
    refs = list(refs)

    def take(count):
        taken = refs[:count]
        del refs[:count]
        return taken

    count = blocks_of(rows)
    block = rows // count
    ahead = min(AHEAD, count)
    me = lax.axis_index("zero")
    used = sorted({t for name in new for t, _, _ in pieces(name, cols)})
    tensors = {t: take(3) for t in used}
    gain_in = take(1)[0] if new else None
    scale_in = {name: (take(1)[0], take(1)[0], take(n - 1)) for name in scaled}
    own_in = {name: take(1)[0] for name in owned}
    finish_in = {name: (take(1)[0] if name[0] == "x" else None, take(n - 1)) for name in finished}
    here_best = [name for name in scaled + finished if name in scaled or name[0] == "x"]
    past = [name for name in last if name not in here_best]
    old_best = dict(zip(past, take(len(past))))
    if with_outs and not fresh:
        take(2)
    gain = gain_in
    if opening:
        gain = take(1)[0]
    made = {name: take(1 if name[0] == "x" else 2) for name in new}
    owns = {name: take(len(SENDS[name])) for name in scaled}
    best = {name: take(1)[0] for name in here_best}
    outs = take(2) if with_outs else None
    fac_out = take(2) if last else None
    total = sum(width(name, cols) for name in new)
    if new:
        raw, load_sem = take(2)
    if opening:
        gain_row, gain_sem = take(2)
    stages = {name: take(1)[0] for name in finished if name[0] == "x"}
    if with_outs:
        out_sem = take(1)[0]
    if last:
        fac, fac_sem = take(2)

    if opening:
        fetch = pltpu.make_async_copy(gain_in, gain_row, gain_sem)
        fetch.start()
    spans = []
    first = 0
    for name in new:
        for t, c0, w in pieces(name, cols):
            if spans and spans[-1][0] == t and spans[-1][1] + spans[-1][2] == c0:
                spans[-1][2] += w
            else:
                spans.append([t, c0, w, first])
            first += w

    def load(j):
        here = pl.ds(j * block, block)
        for name in new:
            own = 0
            for t, c0, w in pieces(name, cols):
                target = made[name][0].at[here, pl.ds(own, w)]
                pltpu.make_async_copy(tensors[t][0].at[here, pl.ds(c0, w)], target, load_sem.at[j]).start()
                own += w
        for t, c0, w, side in spans:
            for k in range(2):
                if 3 * t + 1 + k in NEAR:
                    continue
                target = raw.at[pl.ds(k * rows + j * block, block), pl.ds(side, w)]
                pltpu.make_async_copy(tensors[t][1 + k].at[here, pl.ds(c0, w)], target, load_sem.at[j]).start()

    if new:
        lax.fori_loop(0, ahead, lambda j, _: (load(j), 0)[1], 0)

    sem_at = 0
    waits = []

    def put(source, row, height, name, sem):
        at = 0
        for t, c0, w in pieces(name, cols):
            pltpu.make_async_copy(
                source.at[:, pl.ds(at, w)], outs[t].at[pl.ds(row, height), pl.ds(c0, w)], out_sem.at[sem]
            ).start()
            at += w

    for name in finished:
        if name[0] == "b":
            for k, other in enumerate(finish_in[name][1]):
                put(other, lax.rem(me + 1 + k, n) * rows, rows, name, sem_at)
                waits.append((other, sem_at))
                sem_at += 1
    for name in scaled:
        x, top, tops = scale_in[name]
        high = top[...]
        for other in tops:
            high = jnp.maximum(high, other[...])
        high = jnp.max(high, axis=0, keepdims=True)
        best[name][...] = jnp.broadcast_to(high, best[name].shape)
        inverse = 1.0 / high

        side = 0
        for target in owns[name]:

            def scale_own(j, _):
                scale_block(j, block, x, side, inverse, target, 0)
                return 0

            lax.fori_loop(0, count, scale_own, 0)
            side += target.shape[1]
    for name in owned:
        put(own_in[name], me * rows, rows, name, sem_at)
        waits.append((own_in[name], sem_at))
        sem_at += 1
    for name in finished:
        if name[0] == "x":
            own, got = finish_in[name]
            sources = [own] + got
            high = own[pl.ds(rows, 8), :]
            for other in got:
                high = jnp.maximum(high, other[pl.ds(rows, 8), :])
            high = jnp.max(high, axis=0, keepdims=True)
            best[name][...] = jnp.broadcast_to(high, best[name].shape)
            inverse = 1.0 / high
            stage = stages[name]
            for s, source in enumerate(sources):

                def scale_both(j, _):
                    scale_block(j, block, source, 0, inverse, stage, s * rows)
                    row = lax.rem(me + s, n) * rows + j * block
                    put(stage.at[pl.ds(s * rows + j * block, block), :], row, block, name, sem_at)
                    return 0

                lax.fori_loop(0, count, scale_both, 0)
            waits.append((stage, sem_at))
            sem_at += 1

    if opening:
        fetch.wait()

        def spread(j, _):
            gain[pl.ds(j * LANES, LANES), :] = jnp.broadcast_to(gain_row[pl.ds(j, 1), :], (LANES, LANES)).T
            return 0

        lax.fori_loop(0, rows // LANES, spread, 0)

    def near_of(name):
        (t, c0, _), *more = pieces(name, cols)
        if 3 * t + 2 not in NEAR:
            return None
        assert not more
        return tensors[t][2], c0

    def one(j, _):
        near = sum(w for t, _, w, _ in spans if 3 * t + 2 in NEAR)
        for wide, lines in ((total - near, 3 * block), (near, 2 * block)):
            if wide:
                whole = raw.at[pl.ds(0, lines), pl.ds(0, wide)]
                pltpu.make_async_copy(whole, whole, load_sem.at[j]).wait()

        @pl.when(j + ahead < count)
        def _():
            load(j + ahead)

        first = 0
        for name in new:
            x = made[name][0]
            top, row = (x, rows) if name[0] == "x" else (made[name][1], 0)
            update_block(j, block, x, top, row, raw, first, rows, gain, near_of(name))
            first += width(name, cols)
        return 0

    if new:
        for name in new:
            top, row = (made[name][0], rows) if name[0] == "x" else (made[name][1], 0)
            top[pl.ds(row, 8), :] = jnp.zeros((8, top.shape[1]), jnp.float32)
        lax.fori_loop(0, count, one, 0)

    for name in last:
        high = best[name] if name in best else old_best[name]
        first = 0
        for t, c0, w in pieces(name, cols):
            for q in range(0, w, LANES):
                row = (c0 + q) // LANES
                fac[t, row : row + 1, :] = high[0:1, first + q : first + q + LANES]
            first += w
    if last:
        fac_copies = [pltpu.make_async_copy(fac.at[t], fac_out[t], fac_sem.at[t]) for t in range(2)]
        for copy in fac_copies:
            copy.start()
        for copy in fac_copies:
            copy.wait()
    for whole, sem in waits:
        pltpu.make_async_copy(whole, whole, out_sem.at[sem]).wait()


def per_device(n, weight_gate, moment_gate, square_gate, weight_up, moment_up, square_up, norm_gain):
    rows, cols = weight_gate.shape
    far = [
        v if k in NEAR else pltpu.with_memory_space_constraint(v, pltpu.HBM)
        for k, v in enumerate((weight_gate, moment_gate, square_gate, weight_up, moment_up, square_up))
    ]
    gain = pltpu.with_memory_space_constraint(norm_gain.reshape(rows // LANES, LANES), pltpu.HBM)
    back = [[(i, (i - k) % n) for i in range(n)] for k in range(1, n)]
    outs = None
    own, top, tops, got, best = {}, {}, {}, {}, {}
    wide = {name: width(name, cols) for name in [*PARTS, *(v for k in SENDS for v in sends(k))]}

    def swap(value):
        return [lax.ppermute(value, "zero", pairs) for pairs in back]

    for s, (new, scaled, owned, finished) in enumerate(STEPS):
        opening = s == 0
        with_outs = bool(owned or finished)
        fresh = outs is None
        last = tuple(PARTS) if s == len(STEPS) - 1 else ()
        args, specs, shapes, scratch, aliases = [], [], [], [], {}

        def add(values, spec):
            args.extend(values)
            specs.extend([spec] * len(values))

        for t in sorted({t for name in new for t, _, _ in pieces(name, cols)}):
            for k in range(3 * t, 3 * t + 3):
                add([far[k]], VM if k in NEAR else HB)
        if new:
            add([gain], HB if opening else VM)
        for name in scaled:
            add([own[name], top[name]] + tops[name], VM)
        add([own[name] for name in owned], VM)
        for name in finished:
            add(([own[name]] if name[0] == "x" else []) + got[name], VM)
        made_here = [name for name in scaled + finished if name in scaled or name[0] == "x"]
        old_best = [name for name in last if name not in made_here]
        add([best[name] for name in old_best], VM)
        if opening:
            shapes.append(pltpu.VMEM((rows, LANES), jnp.float32))
        for name in new:
            if name[0] == "x":
                shapes.append(pltpu.VMEM((rows + 8, wide[name]), jnp.float32))
            else:
                shapes.append(pltpu.VMEM((rows, wide[name]), jnp.float32))
                shapes.append(pltpu.VMEM((8, wide[name]), jnp.float32))
        shapes += [pltpu.VMEM((rows, wide[send]), jnp.bfloat16) for name in scaled for send in sends(name)]
        shapes += [pltpu.VMEM((8, wide[name]), jnp.float32) for name in made_here]
        out_specs = [VM] * len(shapes)
        total = sum(wide[name] for name in new)
        room = 2
        if new:
            scratch += [pltpu.VMEM((2 * rows, total), jnp.float32), pltpu.SemaphoreType.DMA((blocks_of(rows),))]
            room += 2 * rows * total * 4 // MIB
        if opening:
            scratch += [pltpu.VMEM((rows // LANES, LANES), jnp.float32), pltpu.SemaphoreType.DMA]
        for name in finished:
            if name[0] == "x":
                scratch.append(pltpu.VMEM((n * rows, wide[name]), jnp.bfloat16))
                room += n * rows * wide[name] * 2 // MIB + 1
        if with_outs:
            count = len(owned) + sum(1 if name[0] == "x" else n - 1 for name in finished)
            scratch.append(pltpu.SemaphoreType.DMA((count,)))
            if not fresh:
                for q in range(2):
                    aliases[len(args) + q] = len(shapes) + q
                add(outs, HB)
            shapes += [jax.ShapeDtypeStruct((n * rows, cols), jnp.bfloat16)] * 2
            out_specs += [HB] * 2
        if last:
            shapes += [jax.ShapeDtypeStruct((cols // LANES, LANES), jnp.float32)] * 2
            out_specs += [HB] * 2
            scratch += [pltpu.VMEM((2, cols // LANES, LANES), jnp.float32), pltpu.SemaphoreType.DMA((2,))]
        result = list(
            pl.pallas_call(
                functools.partial(
                    step, n, rows, cols, (new, scaled, owned, finished), (opening, with_outs, fresh, last)
                ),
                out_shape=shapes,
                in_specs=specs,
                out_specs=out_specs,
                scratch_shapes=scratch,
                input_output_aliases=aliases,
                cost_estimate=pl.CostEstimate(flops=10**8, bytes_accessed=16 * MIB, transcendentals=0),
                compiler_params=pltpu.CompilerParams(vmem_limit_bytes=room * MIB),
            )(*args)
        )
        if opening:
            gain = result.pop(0)
        for name in new:
            own[name] = result.pop(0)
            if name[0] == "b":
                top[name] = result.pop(0)
                tops[name] = swap(top[name])
            else:
                got[name] = swap(own[name])
        for name in scaled:
            for send in sends(name):
                own[send] = result.pop(0)
                got[send] = swap(own[send])
        for name in made_here:
            best[name] = result.pop(0)
        if with_outs:
            outs = [result.pop(0), result.pop(0)]
    return (outs[0], outs[1], result[0].reshape(-1), result[1].reshape(-1))


def solution(mesh):
    def body(*values):
        return per_device(mesh.shape["zero"], *values)

    split = P(("ens", "zero"), "cols")
    return jax.shard_map(
        body,
        mesh=mesh,
        in_specs=(split,) * 6 + (P(("ens", "zero")),),
        out_specs=(P("ens", "cols"), P("ens", "cols"), P(("ens", "cols")), P(("ens", "cols"))),
        check_vma=False,
    )
```

```python
import functools

import jax
import jax.numpy as jnp
from jax import lax
from jax.experimental import pallas as pl
from jax.experimental.pallas import tpu as pltpu
from jax.sharding import PartitionSpec as P


learn_rate = 0.2
hold_rate = 0.9
LANES = 128
BLOCKS = 16
ROWS = 16
GROUP = 512
AHEAD = 16
NEAR = (5,)
MIB = 2**20
VM = pl.BlockSpec(memory_space=pltpu.VMEM)
HB = pl.BlockSpec(memory_space=pltpu.HBM)

PARTS = {
    "x0a": ((0, 0, 8),),
    "x0b": ((0, 8, 8),),
    "x1": ((1, 0, 2),),
    "b1": ((1, 2, 14),),
}
SENDS = {"b1": (9, 5)}
STEPS = (
    (("x0a",), (), (), ()),
    (("x0b",), (), (), ()),
    (("x1", "b1"), (), (), ()),
    ((), ("b1",), (), ()),
    ((), (), ("b1.0", "b1.1"), ("x0a", "x0b")),
    ((), (), (), ("x1", "b1.0")),
    ((), (), (), ("b1.1",)),
)


def sends(name):
    return [f"{name}.{k}" for k in range(len(SENDS[name]))]


def pieces(name, cols):
    unit = cols // 16
    part, _, k = name.partition(".")
    spans = PARTS[part]
    if k:
        skip, left, spans = sum(SENDS[part][: int(k)]), SENDS[part][int(k)], []
        for t, a, w in PARTS[part]:
            gone = min(skip, w)
            kept = min(left, w - gone)
            skip, left = skip - gone, left - kept
            if kept:
                spans.append((t, a + gone, kept))
    return [(t, a * unit, w * unit) for t, a, w in spans]


def width(name, cols):
    return sum(w for _, _, w in pieces(name, cols))


def blocks_of(rows):
    return min(BLOCKS, rows // ROWS)


def groups(w):
    return [(q, min(GROUP, w - q)) for q in range(0, w, GROUP)]


def loop(count, body, init):
    return lax.fori_loop(0, count, body, init, unroll=min(8, count))


def update_block(j, block, x, side, count, top, top_row, raw, first, rows, gain, near):
    for q, size in groups(count):
        lanes = pl.ds(side + q, size)
        wide = pl.ds(first + q, size)

        def body(i, high):
            r = pl.multiple_of(j * block + i * 8, 8)
            at = (pl.ds(r, 8), lanes)
            scale = jnp.concatenate([gain[pl.ds(r, 8), :]] * (size // LANES), axis=1)
            if near is None:
                square = raw[pl.ds(rows + r, 8), wide]
            else:
                square = near[0][pl.ds(r, 8), pl.ds(near[1] + q, size)]
            hold = hold_rate * raw[pl.ds(r, 8), wide] + square
            value = (x[at] - learn_rate * hold) * scale
            x[at] = value
            return jnp.maximum(high, jnp.abs(value))

        top[pl.ds(top_row, 8), lanes] = loop(block // 8, body, top[pl.ds(top_row, 8), lanes])


def scale_block(j, block, source, side, inverse, target, first):
    for q, size in groups(target.shape[1]):
        lanes = pl.ds(q, size)
        wide = pl.ds(side + q, size)
        scale = jnp.broadcast_to(inverse[:, side + q : side + q + size], (16, size))

        def body(i, _):
            r = pl.multiple_of(j * block + i * 16, 16)
            target[pl.ds(first + r, 16), lanes] = (source[pl.ds(r, 16), wide] * scale).astype(target.dtype)
            return 0

        loop(block // 16, body, 0)


def step(n, rows, cols, plan, flags, *refs):
    new, scaled, owned, finished = plan
    opening, with_outs, fresh, last = flags
    refs = list(refs)

    def take(count):
        taken = refs[:count]
        del refs[:count]
        return taken

    count = blocks_of(rows)
    block = rows // count
    ahead = min(AHEAD, count)
    me = lax.axis_index("zero")
    used = sorted({t for name in new for t, _, _ in pieces(name, cols)})
    tensors = {t: take(3) for t in used}
    gain_in = take(1)[0] if new else None
    scale_in = {name: (take(1)[0], take(1)[0], take(n - 1)) for name in scaled}
    own_in = {name: take(1)[0] for name in owned}
    finish_in = {name: (take(1)[0] if name[0] == "x" else None, take(n - 1)) for name in finished}
    here_best = [name for name in scaled + finished if name in scaled or name[0] == "x"]
    past = [name for name in last if name not in here_best]
    old_best = dict(zip(past, take(len(past))))
    if with_outs and not fresh:
        take(2)
    gain = gain_in
    if opening:
        gain = take(1)[0]
    made = {name: take(1 if name[0] == "x" else 2) for name in new}
    owns = {name: take(len(SENDS[name])) for name in scaled}
    best = {name: take(1)[0] for name in here_best}
    outs = take(2) if with_outs else None
    fac_out = take(2) if last else None
    total = sum(width(name, cols) for name in new)
    if new:
        raw, load_sem = take(2)
    if opening:
        gain_row, gain_sem = take(2)
    stages = {name: take(1)[0] for name in finished if name[0] == "x"}
    if with_outs:
        out_sem = take(1)[0]
    if last:
        fac, fac_sem = take(2)

    if opening:
        fetch = pltpu.make_async_copy(gain_in, gain_row, gain_sem)
        fetch.start()
    spans = []
    first = 0
    for name in new:
        for t, c0, w in pieces(name, cols):
            if spans and spans[-1][0] == t and spans[-1][1] + spans[-1][2] == c0:
                spans[-1][2] += w
            else:
                spans.append([t, c0, w, first])
            first += w

    def load(j):
        here = pl.ds(j * block, block)
        for name in new:
            own = 0
            for t, c0, w in pieces(name, cols):
                target = made[name][0].at[here, pl.ds(own, w)]
                pltpu.make_async_copy(tensors[t][0].at[here, pl.ds(c0, w)], target, load_sem.at[j]).start()
                own += w
        for t, c0, w, side in spans:
            for k in range(2):
                if 3 * t + 1 + k in NEAR:
                    continue
                target = raw.at[pl.ds(k * rows + j * block, block), pl.ds(side, w)]
                pltpu.make_async_copy(tensors[t][1 + k].at[here, pl.ds(c0, w)], target, load_sem.at[j]).start()

    if new:
        lax.fori_loop(0, ahead, lambda j, _: (load(j), 0)[1], 0)

    sem_at = 0
    waits = []

    def put(source, row, height, name, sem):
        at = 0
        for t, c0, w in pieces(name, cols):
            pltpu.make_async_copy(
                source.at[:, pl.ds(at, w)], outs[t].at[pl.ds(row, height), pl.ds(c0, w)], out_sem.at[sem]
            ).start()
            at += w

    for name in finished:
        if name[0] == "b":
            for k, other in enumerate(finish_in[name][1]):
                put(other, lax.rem(me + 1 + k, n) * rows, rows, name, sem_at)
                waits.append((other, sem_at))
                sem_at += 1
    for name in scaled:
        x, top, tops = scale_in[name]
        high = top[...]
        for other in tops:
            high = jnp.maximum(high, other[...])
        high = jnp.max(high, axis=0, keepdims=True)
        best[name][...] = jnp.broadcast_to(high, best[name].shape)
        inverse = 1.0 / high

        side = 0
        for target in owns[name]:

            def scale_own(j, _):
                scale_block(j, block, x, side, inverse, target, 0)
                return 0

            lax.fori_loop(0, count, scale_own, 0)
            side += target.shape[1]
    for name in owned:
        put(own_in[name], me * rows, rows, name, sem_at)
        waits.append((own_in[name], sem_at))
        sem_at += 1
    for name in finished:
        if name[0] == "x":
            own, got = finish_in[name]
            sources = [own] + got
            high = own[pl.ds(rows, 8), :]
            for other in got:
                high = jnp.maximum(high, other[pl.ds(rows, 8), :])
            high = jnp.max(high, axis=0, keepdims=True)
            best[name][...] = jnp.broadcast_to(high, best[name].shape)
            inverse = 1.0 / high
            stage = stages[name]
            for s, source in enumerate(sources):

                def scale_both(j, _):
                    scale_block(j, block, source, 0, inverse, stage, s * rows)
                    row = lax.rem(me + s, n) * rows + j * block
                    put(stage.at[pl.ds(s * rows + j * block, block), :], row, block, name, sem_at)
                    return 0

                lax.fori_loop(0, count, scale_both, 0)
            waits.append((stage, sem_at))
            sem_at += 1

    if opening:
        fetch.wait()

        def spread(j, _):
            gain[pl.ds(j * LANES, LANES), :] = jnp.broadcast_to(gain_row[pl.ds(j, 1), :], (LANES, LANES)).T
            return 0

        lax.fori_loop(0, rows // LANES, spread, 0)

    def one(j, _):
        near = sum(w for t, _, w, _ in spans if 3 * t + 2 in NEAR)
        for wide, lines in ((total - near, 3 * block), (near, 2 * block)):
            if wide:
                whole = raw.at[pl.ds(0, lines), pl.ds(0, wide)]
                pltpu.make_async_copy(whole, whole, load_sem.at[j]).wait()

        @pl.when(j + ahead < count)
        def _():
            load(j + ahead)

        first = 0
        for name in new:
            x = made[name][0]
            top, row = (x, rows) if name[0] == "x" else (made[name][1], 0)
            side = 0
            for t, c0, w in pieces(name, cols):
                near = (tensors[t][2], c0) if 3 * t + 2 in NEAR else None
                update_block(j, block, x, side, w, top, row, raw, first, rows, gain, near)
                side += w
                first += w
        return 0

    if new:
        for name in new:
            top, row = (made[name][0], rows) if name[0] == "x" else (made[name][1], 0)
            top[pl.ds(row, 8), :] = jnp.zeros((8, top.shape[1]), jnp.float32)
        lax.fori_loop(0, count, one, 0)

    for name in last:
        high = best[name] if name in best else old_best[name]
        first = 0
        for t, c0, w in pieces(name, cols):
            for q in range(0, w, LANES):
                row = (c0 + q) // LANES
                fac[t, row : row + 1, :] = high[0:1, first + q : first + q + LANES]
            first += w
    if last:
        fac_copies = [pltpu.make_async_copy(fac.at[t], fac_out[t], fac_sem.at[t]) for t in range(2)]
        for copy in fac_copies:
            copy.start()
        for copy in fac_copies:
            copy.wait()
    for whole, sem in waits:
        pltpu.make_async_copy(whole, whole, out_sem.at[sem]).wait()


def per_device(n, weight_gate, moment_gate, square_gate, weight_up, moment_up, square_up, norm_gain):
    rows, cols = weight_gate.shape
    far = [
        v if k in NEAR else pltpu.with_memory_space_constraint(v, pltpu.HBM)
        for k, v in enumerate((weight_gate, moment_gate, square_gate, weight_up, moment_up, square_up))
    ]
    gain = pltpu.with_memory_space_constraint(norm_gain.reshape(rows // LANES, LANES), pltpu.HBM)
    back = [[(i, (i - k) % n) for i in range(n)] for k in range(1, n)]
    outs = None
    own, top, tops, got, best = {}, {}, {}, {}, {}
    wide = {name: width(name, cols) for name in [*PARTS, *(v for k in SENDS for v in sends(k))]}

    def swap(value):
        return [lax.ppermute(value, "zero", pairs) for pairs in back]

    for s, (new, scaled, owned, finished) in enumerate(STEPS):
        opening = s == 0
        with_outs = bool(owned or finished)
        fresh = outs is None
        last = tuple(PARTS) if s == len(STEPS) - 1 else ()
        args, specs, shapes, scratch, aliases = [], [], [], [], {}

        def add(values, spec):
            args.extend(values)
            specs.extend([spec] * len(values))

        for t in sorted({t for name in new for t, _, _ in pieces(name, cols)}):
            for k in range(3 * t, 3 * t + 3):
                add([far[k]], VM if k in NEAR else HB)
        if new:
            add([gain], HB if opening else VM)
        for name in scaled:
            add([own[name], top[name]] + tops[name], VM)
        add([own[name] for name in owned], VM)
        for name in finished:
            add(([own[name]] if name[0] == "x" else []) + got[name], VM)
        made_here = [name for name in scaled + finished if name in scaled or name[0] == "x"]
        old_best = [name for name in last if name not in made_here]
        add([best[name] for name in old_best], VM)
        if opening:
            shapes.append(pltpu.VMEM((rows, LANES), jnp.float32))
        for name in new:
            if name[0] == "x":
                shapes.append(pltpu.VMEM((rows + 8, wide[name]), jnp.float32))
            else:
                shapes.append(pltpu.VMEM((rows, wide[name]), jnp.float32))
                shapes.append(pltpu.VMEM((8, wide[name]), jnp.float32))
        shapes += [pltpu.VMEM((rows, wide[send]), jnp.bfloat16) for name in scaled for send in sends(name)]
        shapes += [pltpu.VMEM((8, wide[name]), jnp.float32) for name in made_here]
        out_specs = [VM] * len(shapes)
        total = sum(wide[name] for name in new)
        room = 2
        if new:
            scratch += [pltpu.VMEM((2 * rows, total), jnp.float32), pltpu.SemaphoreType.DMA((blocks_of(rows),))]
            room += 2 * rows * total * 4 // MIB
        if opening:
            scratch += [pltpu.VMEM((rows // LANES, LANES), jnp.float32), pltpu.SemaphoreType.DMA]
        for name in finished:
            if name[0] == "x":
                scratch.append(pltpu.VMEM((n * rows, wide[name]), jnp.bfloat16))
                room += n * rows * wide[name] * 2 // MIB + 1
        if with_outs:
            count = len(owned) + sum(1 if name[0] == "x" else n - 1 for name in finished)
            scratch.append(pltpu.SemaphoreType.DMA((count,)))
            if not fresh:
                for q in range(2):
                    aliases[len(args) + q] = len(shapes) + q
                add(outs, HB)
            shapes += [jax.ShapeDtypeStruct((n * rows, cols), jnp.bfloat16)] * 2
            out_specs += [HB] * 2
        if last:
            shapes += [jax.ShapeDtypeStruct((cols // LANES, LANES), jnp.float32)] * 2
            out_specs += [HB] * 2
            scratch += [pltpu.VMEM((2, cols // LANES, LANES), jnp.float32), pltpu.SemaphoreType.DMA((2,))]
        result = list(
            pl.pallas_call(
                functools.partial(
                    step, n, rows, cols, (new, scaled, owned, finished), (opening, with_outs, fresh, last)
                ),
                out_shape=shapes,
                in_specs=specs,
                out_specs=out_specs,
                scratch_shapes=scratch,
                input_output_aliases=aliases,
                cost_estimate=pl.CostEstimate(flops=10**8, bytes_accessed=16 * MIB, transcendentals=0),
                compiler_params=pltpu.CompilerParams(vmem_limit_bytes=room * MIB),
            )(*args)
        )
        if opening:
            gain = result.pop(0)
        for name in new:
            own[name] = result.pop(0)
            if name[0] == "b":
                top[name] = result.pop(0)
                tops[name] = swap(top[name])
            else:
                got[name] = swap(own[name])
        for name in scaled:
            for send in sends(name):
                own[send] = result.pop(0)
                got[send] = swap(own[send])
        for name in made_here:
            best[name] = result.pop(0)
        if with_outs:
            outs = [result.pop(0), result.pop(0)]
    return (outs[0], outs[1], result[0].reshape(-1), result[1].reshape(-1))


def solution(mesh):
    def body(*values):
        return per_device(mesh.shape["zero"], *values)

    split = P(("ens", "zero"), "cols")
    return jax.shard_map(
        body,
        mesh=mesh,
        in_specs=(split,) * 6 + (P(("ens", "zero")),),
        out_specs=(P("ens", "cols"), P("ens", "cols"), P(("ens", "cols")), P(("ens", "cols"))),
        check_vma=False,
    )
```
